32 devices in a mesh: orb: 8 (over z, y), row: 4 (over x, core).
Axes of the slice: x: 2, y: 2, z: 4, core: 2. Of those that a mesh axis runs over, the one named last changes fastest.
Arguments:
- half_ints: bfloat16 [64, 2048, 1536], P(('orb', 'row')), may hold values from -0.125 to 0.125
- metric_inv: bfloat16 [128, 128, 128], P(('orb', 'row')), may hold values from -0.1 to 1.4, as said below
- coefficients: bfloat16 [4096, 64], P(('orb', 'row')), may hold values from -0.15625 to 0.15625
- basis_domain: int32 [64, 12], P(('orb', 'row')), may hold values from 0 to 31, as said below
- aux_domain: int32 [64, 16], P(('orb', 'row')), may hold values from 0 to 127, as said below
- aux_count: int32 [64], P(('orb', 'row')), may hold values from 8 to 16, as said below
Outputs:
- exchange_matrix: float32 [4096, 4096], P(('orb', 'row'))
- self_energy: float32 [], replicated
The draws below stay inside these ranges and needn't reach their ends.
Inputs may be any that keep to these rules, and one draw needn't show every extreme that they name: `metric_inv`: each block is lower triangular. `basis_domain`: each row names 12 different basis blocks. Among the 2 rows of one device (rows d * 2 to (d + 1) * 2 - 1), no basis block is named by more than 1 row (the two orbitals' domains are disjoint). `aux_domain`: each row names 16 different auxiliary blocks. Orbital i uses the first aux_count[i] blocks of its list; some orbital uses all 16.
All inputs are finite; a program needn't handle non-finite values.
Results may differ from the reference program's by a relative error of at most 0.00079.
Values may be sent and summed in bfloat16 or wider, within the bound.
No kernel may reach another device: no remote copies, remote signals or barrier semaphores. Data moves between devices by JAX's collectives and lax.ppermute only.
A program may use at most 128 MiB of HBM per device.

```python
import jax
import jax.numpy as jnp
from jax import lax

BLK = 128
NBB = 32
NAB = 128
NBD = 12
NAD = 16
ORB_DEV = 2
NOCC = 64
NB = 4096


def distinct_blocks(key, row_count, picked, available):
    scores = jax.random.randint(key, (row_count, available), 0, 1048576) * available
    scores = scores + jnp.arange(available, dtype=jnp.int32)[None, :]
    ranking = jnp.argsort(scores, axis=1)
    return ranking[:, :picked].astype(jnp.int32)


def draw_basis_domain(key, part):
    groups = NOCC // ORB_DEV
    order = distinct_blocks(jax.random.fold_in(key, 11), groups, NBB, NBB)
    positions = (jnp.arange(ORB_DEV, dtype=jnp.int32)[:, None] * NBD + jnp.arange(NBD, dtype=jnp.int32)[None, :]) % NBB
    picked = order[:, positions.reshape(-1)]
    return picked.reshape(NOCC, NBD).astype(jnp.int32)


def draw_aux_domain(key, part):
    return distinct_blocks(jax.random.fold_in(key, 12), NOCC, NAD, NAB)


def draw_aux_count(key, part):
    subkeys = jax.random.split(jax.random.fold_in(key, 13), 3)
    half_count = NAD // 2
    draw_one = jax.random.randint(subkeys[0], (NOCC,), 0, NAD)
    draw_two = jax.random.randint(subkeys[1], (NOCC,), 0, NAD)
    counts = half_count + draw_one * draw_two * (NAD - half_count) // (NAD - 1) ** 2
    chosen = jax.random.randint(subkeys[2], (), 0, NOCC)
    return counts.at[chosen].set(NAD).astype(jnp.int32)


def draw_metric_inv(key, part):
    subkeys = jax.random.split(jax.random.fold_in(key, 14), 2)
    diagonal = jax.random.uniform(subkeys[0], (NAB, BLK), jnp.float32, 0.8, 1.2)
    strict_part = jax.random.uniform(subkeys[1], (NAB, BLK, BLK), jnp.float32, -0.099, 0.099)
    positions = jnp.arange(BLK)
    below_mask = (positions[:, None] > positions[None, :]).astype(jnp.float32)
    on_diagonal = (positions[:, None] == positions[None, :]).astype(jnp.float32)
    return (strict_part * below_mask + diagonal[:, :, None] * on_diagonal).astype(jnp.bfloat16)


def level_of(rng, shape, pieces, least, top_value):
    level = 1.0
    for axis_at, blocks in pieces:
        heights = jax.random.uniform(jax.random.fold_in(jax.random.fold_in(rng, 6), axis_at), (blocks,), jnp.float32, least / len(pieces), top_value / len(pieces))
        level = level * jnp.repeat(jnp.exp(heights), shape[axis_at] // blocks).reshape((-1,) + (1,) * (len(shape) - 1 - axis_at))
    return level


def centred(rng, extent, deviation, reach, shards=(), kind=jnp.bfloat16):
    array = deviation * jax.random.normal(rng, extent, jnp.float32)
    if shards:
        array = array * level_of(rng, extent, shards, -0.22, 0.18)
    return jnp.clip(array, -reach, reach).astype(kind)


def setup_inputs(seed: int = 0) -> dict:
    key_of = jax.random.split(jax.random.key(seed), 7)
    half_ints = centred(key_of[0], (NOCC, NAD * BLK, NBD * BLK), (NAD * BLK) ** -0.5, 0.125, ((0, 32),))
    metric_inv = draw_metric_inv(jax.random.fold_in(key_of[6], 71), 0)
    coefficients = centred(key_of[2], (NB, NOCC), (NBD * BLK) ** -0.5, 0.15625, ((0, 32),))
    basis_domain = draw_basis_domain(jax.random.fold_in(key_of[6], 71), 0)
    aux_domain = draw_aux_domain(jax.random.fold_in(key_of[6], 71), 0)
    aux_count = draw_aux_count(jax.random.fold_in(key_of[6], 71), 0)
    return {"half_ints": half_ints, "metric_inv": metric_inv, "coefficients": coefficients, "basis_domain": basis_domain, "aux_domain": aux_domain, "aux_count": aux_count}


def fit_orbital(block_rows, aux_ids, live_count, basis_ids, coef_column, metric_inv):
    block_width = metric_inv.shape[1]
    columns = block_rows.shape[1]
    group_size = min(4, NAD)
    coef_domain = coef_column.reshape(NBB, block_width)[basis_ids].reshape(-1).astype(jnp.float32)
    group_total = (live_count + group_size - 1) // group_size

    def advance(group_index, carry):
        k_partial, energy = carry
        first_block = group_index * group_size
        rows_now = lax.dynamic_slice_in_dim(block_rows, first_block * block_width, group_size * block_width, 0)
        rows_now = rows_now.astype(jnp.float32).reshape(group_size, block_width, columns)
        block_ids = lax.dynamic_slice_in_dim(aux_ids, first_block, group_size, 0)
        factors = metric_inv[block_ids].astype(jnp.float32)
        fitted = jnp.einsum("gqp,gpm->gqm", factors, rows_now, precision=lax.Precision.HIGHEST).astype(jnp.bfloat16)
        live_mask = (first_block + jnp.arange(group_size, dtype=jnp.int32)) < live_count
        fitted = jnp.where(live_mask[:, None, None], fitted, jnp.zeros_like(fitted))
        flat_rows = fitted.astype(jnp.float32).reshape(group_size * block_width, columns)
        k_partial = k_partial + jnp.dot(flat_rows.T, flat_rows, precision=lax.Precision.HIGHEST)
        projected = jnp.dot(flat_rows, coef_domain, precision=lax.Precision.HIGHEST)
        return k_partial, energy + jnp.sum(projected * projected)

    initial = (jnp.zeros((columns, columns), jnp.float32), jnp.zeros((), jnp.float32))
    return lax.fori_loop(0, group_total, advance, initial)


def reference(half_ints, metric_inv, coefficients, basis_domain, aux_domain, aux_count):
    block_width = metric_inv.shape[1]
    count_blocks = basis_domain.shape[1]

    def one_orbital(orbital, carry):
        k_whole, energy_sum = carry
        k_partial, energy = fit_orbital(half_ints[orbital], aux_domain[orbital], aux_count[orbital],
                                        basis_domain[orbital], coefficients[:, orbital], metric_inv)
        rounded = lax.optimization_barrier(k_partial.astype(jnp.bfloat16)).astype(jnp.float32)
        k_tiles = rounded.reshape(count_blocks, block_width, count_blocks, block_width).transpose(0, 2, 1, 3)
        block_ids = basis_domain[orbital]
        k_whole = k_whole.at[block_ids[:, None], :, block_ids[None, :], :].add(k_tiles)
        return k_whole, energy_sum + energy

    initial = (jnp.zeros((NBB, block_width, NBB, block_width), jnp.float32), jnp.zeros((), jnp.float32))
    k_whole, energy_sum = lax.fori_loop(0, NOCC, one_orbital, initial)
    return k_whole.reshape(NB, NB), energy_sum / NOCC
```

```python
import jax
import jax.numpy as jnp
from jax import lax
from jax.experimental import pallas as pl
from jax.experimental.pallas import tpu as pltpu
from jax.sharding import Mesh
from jax.sharding import PartitionSpec as P

AXES = ("h", "u", "v", "r", "c")
LINE = ("h", "u")
GROUP = ("u", "v", "r", "c")
TAIL = 8
STEP = 4
TOP = 32000.0


def xor_permute(value, axes, size, offset):
    return lax.ppermute(value, axes, [(i, i ^ offset) for i in range(size)])


def pack_metric(metric, domain):
    count, width, _ = metric.shape
    row = lax.broadcasted_iota(jnp.int32, (width, width), 0)
    col = lax.broadcasted_iota(jnp.int32, (width, width), 1)
    if count % 2 == 0:
        first, second = metric[: count // 2], metric[count // 2 :]
        packed = jnp.where(row >= col, first, jnp.swapaxes(second, 1, 2))
        diagonal = jnp.sum(jnp.where(row == col, second, jnp.zeros_like(second)), axis=1)
    else:
        packed = metric
        diagonal = jnp.zeros((count, width), metric.dtype)
    ids = domain.reshape(1, -1)
    ids = jnp.pad(ids, ((0, 0), (0, width - ids.shape[1])))
    ids = jnp.broadcast_to(ids, (packed.shape[0], width))
    extra = jnp.stack([diagonal, (ids // width).astype(metric.dtype), (ids % width).astype(metric.dtype)], 1)
    extra = jnp.pad(extra, ((0, 0), (0, TAIL - 3), (0, 0)))
    return jnp.concatenate([packed, extra], 1)


def fit_kernel(orbitals, positions, listed, pack_count, halves_packed, line, mid, group_blocks, width):
    windows = positions // 2 + 1
    group_total = listed // STEP
    order = positions * width
    block = windows * width

    def body(aux_ref, count_ref, domain_ref, place_ref, *refs):
        parts = refs[: 2 * mid]
        rows_ref, coef_ref, out_other, out_own, energy_ref = refs[2 * mid : 2 * mid + 5]
        metric, fitted, total, stage, gather_sems, out_sems = refs[2 * mid + 5 :]
        orbital = pl.program_id(0)
        group = pl.program_id(1)
        part = line * pack_count

        @pl.when((orbital == 0) & (group == 0))
        def _():
            copies = [
                pltpu.make_async_copy(parts[i], metric.at[pl.ds(i * part, part)], gather_sems.at[i])
                for i in range(2 * mid)
            ]
            for copy in copies:
                copy.start()
            for copy in copies:
                copy.wait()

        live = count_ref[orbital]
        row = lax.broadcasted_iota(jnp.int32, (width, width), 0)
        col = lax.broadcasted_iota(jnp.int32, (width, width), 1)

        @pl.when(group * STEP < live)
        def _():
            for j in range(STEP):
                listed_at = group * STEP + j
                base = pl.multiple_of(listed_at * width, width)

                @pl.when(listed_at < live)
                def _():
                    aux = aux_ref[orbital, listed_at]
                    per_device = pack_count * (2 if halves_packed else 1)
                    owner = aux // per_device
                    inner = aux - owner * per_device
                    away = owner ^ place_ref[0]
                    core = away % 2
                    between = (away // 2) % mid
                    along = away // (2 * mid)
                    slot = inner % pack_count
                    at = ((core * mid + between) * line + along) * pack_count + slot
                    square = metric[at, :width, :].astype(jnp.float32)
                    lower = jnp.where(row >= col, square, 0.0)
                    if halves_packed:
                        extra = metric[at, width : width + TAIL, :].astype(jnp.float32)
                        upper = jnp.where(row > col, square.T, 0.0)
                        upper = jnp.where(row == col, extra[0:1, :], upper)
                        lower = jnp.where(inner >= pack_count, upper, lower)
                    fit = jnp.dot(
                        lower.astype(jnp.bfloat16),
                        rows_ref[0, j * width : (j + 1) * width, :],
                        preferred_element_type=jnp.float32,
                    ).astype(jnp.bfloat16)
                    fitted[pl.ds(base, width), :order] = fit
                    fitted[pl.ds(base, width), order:] = fit[:, : windows * width]

                @pl.when(listed_at >= live)
                def _():
                    fitted[pl.ds(base, width), :] = jnp.zeros((width, order + windows * width), jnp.bfloat16)

        @pl.when(group == group_total - 1)
        def _():
            steps = (live + STEP - 1) // STEP
            depth = STEP * width
            ones = jnp.ones((width, width), jnp.bfloat16)
            energy = jnp.zeros((width, width), jnp.float32)
            for pair in range(positions // 2):
                left = pair * 2 * width
                total[...] = jnp.zeros_like(total)

                def accumulate(k, carry):
                    at = pl.multiple_of(k * depth, depth)
                    total[...] += lax.dot_general(
                        fitted[pl.ds(at, depth), left : left + 2 * width],
                        fitted[pl.ds(at, depth), left : left + block + width],
                        (((0,), (0,)), ((), ())),
                        preferred_element_type=jnp.float32,
                    )
                    return carry

                lax.fori_loop(0, steps, accumulate, 0)
                for half in range(2):
                    place = 2 * pair + half
                    values = total[half * width : (half + 1) * width, half * width : half * width + block]
                    mixed = jnp.zeros((width, width), jnp.float32)
                    for w in range(windows):
                        basis = domain_ref[orbital, (place + w) % positions]
                        once = w == 0 or 2 * w == positions
                        line_coef = coef_ref[orbital, pl.ds(basis, 1), :] * (1.0 if once else 2.0)
                        mixed += values[:, w * width : (w + 1) * width] * line_coef
                    basis = domain_ref[orbital, place]
                    spread = jnp.where(row == col, coef_ref[orbital, pl.ds(basis, 1), :], 0.0)
                    spread = jnp.dot(spread.astype(jnp.bfloat16), ones, preferred_element_type=jnp.float32)
                    energy += mixed * spread
                    other = basis // group_blocks != place_ref[1]
                    target = basis % group_blocks
                    slot = half

                    def drain():
                        pltpu.make_async_copy(stage.at[slot], out_own.at[0], out_sems.at[slot]).wait()

                    if pair == 0:
                        pl.when(orbital > 0)(drain)
                    else:
                        drain()
                    stage[slot] = values.astype(jnp.bfloat16)

                    @pl.when(other)
                    def _():
                        pltpu.make_async_copy(stage.at[slot], out_other.at[target], out_sems.at[slot]).start()

                    @pl.when(jnp.logical_not(other))
                    def _():
                        pltpu.make_async_copy(stage.at[slot], out_own.at[target], out_sems.at[slot]).start()

            @pl.when(orbital == 0)
            def _():
                energy_ref[...] = jnp.zeros_like(energy_ref)

            energy_ref[...] += energy

            @pl.when(orbital == orbitals - 1)
            def _():
                for slot in range(2):
                    pltpu.make_async_copy(stage.at[slot], out_own.at[0], out_sems.at[slot]).wait()

    return body


def fit_call(half_ints, aux_domain, aux_count, basis_domain, place, parts, coef, group_blocks, halves_packed, line, mid):
    orbitals, rows, order = half_ints.shape
    listed = aux_domain.shape[1]
    positions = basis_domain.shape[1]
    width = order // positions
    windows = positions // 2 + 1
    pack_count = parts[0].shape[0] // line
    pack_rows = parts[0].shape[1]

    def rows_map(o, g, aux, count, domain, here):
        return (o, jnp.minimum(g, jnp.maximum((count[o] + STEP - 1) // STEP - 1, 0)), 0)

    return pl.pallas_call(
        fit_kernel(orbitals, positions, listed, pack_count, halves_packed, line, mid, group_blocks, width),
        out_shape=(
            jax.ShapeDtypeStruct((group_blocks, width, windows * width), jnp.bfloat16),
            jax.ShapeDtypeStruct((group_blocks, width, windows * width), jnp.bfloat16),
            jax.ShapeDtypeStruct((width, width), jnp.float32),
        ),
        grid_spec=pltpu.PrefetchScalarGridSpec(
            num_scalar_prefetch=4,
            grid=(orbitals, listed // STEP),
            in_specs=[pl.BlockSpec(memory_space=pl.ANY)] * len(parts)
            + [
                pl.BlockSpec((1, STEP * width, order), rows_map),
                pl.BlockSpec(coef.shape, lambda o, g, *_: (0, 0, 0)),
            ],
            out_specs=(
                pl.BlockSpec(memory_space=pl.ANY),
                pl.BlockSpec(memory_space=pl.ANY),
                pl.BlockSpec((width, width), lambda o, g, *_: (0, 0)),
            ),
            scratch_shapes=[
                pltpu.VMEM((len(parts) * line * pack_count, pack_rows, width), jnp.bfloat16),
                pltpu.VMEM((rows, order + windows * width), jnp.bfloat16),
                pltpu.VMEM((2 * width, (windows + 1) * width), jnp.float32),
                pltpu.VMEM((2, width, windows * width), jnp.bfloat16),
                pltpu.SemaphoreType.DMA((len(parts),)),
                pltpu.SemaphoreType.DMA((2,)),
            ],
        ),
        compiler_params=pltpu.CompilerParams(
            dimension_semantics=("arbitrary", "arbitrary"), vmem_limit_bytes=48 * 2**20
        ),
        name="fit",
    )(aux_domain, aux_count, basis_domain, place, *parts, half_ints, coef)


def encode(values):
    height = jnp.max(jnp.abs(values), axis=0, keepdims=True)
    level = jnp.ceil(8.0 * jnp.log2(jnp.maximum(height, 1e-30) / TOP))
    codes = jnp.round(values * jnp.exp2(level * -0.125))
    return codes.astype(jnp.int32).astype(jnp.int16), level


def decode(codes, level):
    return codes.astype(jnp.int32).astype(jnp.float32) * jnp.exp2(level * 0.125)


def sum_kernel(final, positions, blocks, rows, width, chunk, steps):
    windows = positions // 2 + 1

    def body(at_ref, domain_ref, arrived, *refs):
        if final:
            partner, energy_in, sums_out, codes_out = refs
            total = sums_out
        else:
            codes_out, total = refs
        step = pl.program_id(0)

        @pl.when(step == 0)
        def _():
            if final:
                for b in range(blocks):
                    level = partner[b, rows : rows + TAIL, :].astype(jnp.int32).astype(jnp.float32)[0:1]
                    total[b] = decode(partner[b, :rows, :], level)
            else:
                total[...] = jnp.zeros_like(total)

        for s in range(chunk):
            source = step * chunk + s
            at = at_ref[source]

            @pl.when(at >= 0)
            def _():
                start = at - at % positions
                place = at % positions
                for w in range(windows):
                    basis = domain_ref[source, start + (place + w) % positions]

                    def add():
                        total[basis] += arrived[s, :, w * width : (w + 1) * width].astype(jnp.float32)

                    if 2 * w == positions:
                        pl.when(2 * place < positions)(add)
                    else:
                        add()

        @pl.when(step == steps - 1)
        def _():
            if final:
                energy = jnp.maximum(jnp.sum(energy_in[...]), 1e-30)
                energy = jnp.full((TAIL, width), energy)
                power = jnp.ceil(jnp.log2(energy))
                scaled = energy * jnp.exp2(-power) * 16384.0
                whole = jnp.floor(scaled)
                rest = jnp.round((scaled - whole) * 16384.0)
                lanes = lax.broadcasted_iota(jnp.int32, (TAIL, width), 1) % rows
                second = jnp.where(lanes == 0, power, jnp.where(lanes == 1, whole, jnp.where(lanes == 2, rest, 0.0)))
            for b in range(blocks):
                codes, level = encode(total[b])
                codes_out[b, :rows, :] = codes
                tail = jnp.broadcast_to(level, (TAIL, width))
                if final:
                    lines = lax.broadcasted_iota(jnp.int32, (TAIL, width), 0)
                    tail = jnp.where(lines == 0, tail, second)
                codes_out[b, rows : rows + TAIL, :] = tail.astype(jnp.int32).astype(jnp.int16)

    return body


def sum_call(arrived, at, domains, positions, blocks, width, partner=None, energy=None):
    sources, rows, span = arrived.shape
    chunk = 4
    steps = sources // chunk
    final = partner is not None
    coded = jax.ShapeDtypeStruct((blocks, rows + TAIL, width), jnp.int16)
    coded_spec = pl.BlockSpec((blocks, rows + TAIL, width), lambda g, *_: (0, 0, 0))
    sums_spec = pl.BlockSpec((blocks, rows, width), lambda g, *_: (0, 0, 0))
    in_specs = [pl.BlockSpec((chunk, rows, span), lambda g, *_: (g, 0, 0))]
    operands = [arrived]
    if final:
        in_specs += [coded_spec, pl.BlockSpec((width, width), lambda g, *_: (0, 0))]
        operands += [partner, energy]
        out_shape = (jax.ShapeDtypeStruct((blocks, rows, width), jnp.float32), coded)
        out_specs = (sums_spec, coded_spec)
        scratch = []
    else:
        out_shape = coded
        out_specs = coded_spec
        scratch = [pltpu.VMEM((blocks, rows, width), jnp.float32)]
    return pl.pallas_call(
        sum_kernel(final, positions, blocks, rows, width, chunk, steps),
        out_shape=out_shape,
        grid_spec=pltpu.PrefetchScalarGridSpec(
            num_scalar_prefetch=2,
            grid=(steps,),
            in_specs=in_specs,
            out_specs=out_specs,
            scratch_shapes=scratch,
        ),
        compiler_params=pltpu.CompilerParams(dimension_semantics=("arbitrary",), vmem_limit_bytes=40 * 2**20),
        name="total" if final else "partial",
    )(at, domains, *operands)


def finish_kernel(blocks, rows, width):
    def body(place_ref, sums, arrived, out_ref, energy_ref):
        energy = jnp.zeros((TAIL, width), jnp.float32)
        for b in range(blocks):
            tail = arrived[b, rows : rows + TAIL, :].astype(jnp.int32).astype(jnp.float32)
            energy += energy_of(tail)
            value = decode(arrived[b, :rows, :], tail[0:1]).T
            value = jnp.where(place_ref[2] == b, 0.0, value)
            out_ref[:, b * width : (b + 1) * width] = sums[b] + value
        energy_ref[...] = energy

    return body


def energy_of(tail):
    return (tail[1:2, 1:2] + tail[1:2, 2:3] / 16384.0) / 16384.0 * jnp.exp2(tail[1:2, 0:1])


def finish_call(place, sums, arrived):
    blocks, rows, width = sums.shape
    return pl.pallas_call(
        finish_kernel(blocks, rows, width),
        out_shape=(
            jax.ShapeDtypeStruct((rows, blocks * width), jnp.float32),
            jax.ShapeDtypeStruct((TAIL, width), jnp.float32),
        ),
        grid_spec=pltpu.PrefetchScalarGridSpec(
            num_scalar_prefetch=1,
            grid=(1,),
            in_specs=[
                pl.BlockSpec(sums.shape, lambda g, *_: (0, 0, 0)),
                pl.BlockSpec(arrived.shape, lambda g, *_: (0, 0, 0)),
            ],
            out_specs=(
                pl.BlockSpec((rows, blocks * width), lambda g, *_: (0, 0)),
                pl.BlockSpec((TAIL, width), lambda g, *_: (0, 0)),
            ),
        ),
        compiler_params=pltpu.CompilerParams(vmem_limit_bytes=40 * 2**20),
        name="finish",
    )(place, sums, arrived)


def finish_plain(place, sums, arrived, span):
    blocks, rows, width = sums.shape
    devices = arrived.shape[0]
    codes = arrived[:, :rows, :].astype(jnp.float32)
    level = arrived[:, rows : rows + 1, :].astype(jnp.float32)
    values = codes * jnp.exp2(level * 0.125)
    values = values.transpose(2, 0, 1).reshape(rows, blocks, width)
    mine = jnp.arange(blocks)[None, :, None] == place[2]
    values = jnp.where(mine, 0.0, values)
    out = (sums.transpose(1, 0, 2) + values).reshape(rows, blocks * width)
    tail = arrived[:, rows + 1, :3].astype(jnp.float32)
    energy = jnp.sum((tail[:, 1] + tail[:, 2] / 16384.0) / 16384.0 * jnp.exp2(tail[:, 0]))
    return out, energy


def program(sizes):
    line = sizes[0] * sizes[1]
    mid = sizes[2] * sizes[3]
    devices = line * mid * sizes[4]
    group = devices // 2

    def per_device(half_ints, metric_inv, coefficients, basis_domain, aux_domain, aux_count):
        orbitals, _, order = half_ints.shape
        positions = basis_domain.shape[1]
        width = metric_inv.shape[1]
        rows = coefficients.shape[0]
        span = width // rows
        blocks = rows * devices // width
        group_blocks = group // span
        me = lax.axis_index(AXES)
        my_half = lax.axis_index("h")
        place = jnp.stack([me, my_half, me // span]).astype(jnp.int32)

        coef = coefficients.astype(jnp.float32).reshape(rows, devices, orbitals).transpose(1, 2, 0)
        coef = lax.all_to_all(coef, AXES, 0, 0, tiled=True)
        coef = coef.transpose(1, 0, 2).reshape(orbitals, blocks, width)

        halves_packed = metric_inv.shape[0] % 2 == 0
        packed = pack_metric(metric_inv, basis_domain)
        stack = jnp.concatenate([packed] + [xor_permute(packed, LINE, line, k) for k in range(1, line)], 0)
        near = [stack] + [xor_permute(stack, ("v", "r"), mid, k) for k in range(1, mid)]
        parts = near + [xor_permute(value, "c", 2, 1) for value in near]

        pack_count = packed.shape[0]
        ids = jnp.stack([value.reshape(line, pack_count, -1, width)[:, 0, width + 1 : width + 3] for value in parts])
        ids = ids[..., : orbitals * positions].astype(jnp.int32)
        ids = ids[:, :, 0] * width + ids[:, :, 1]
        ids = ids.reshape(2, mid, line, -1).transpose(2, 1, 0, 3).reshape(devices, -1)
        inside = jnp.arange(group, dtype=jnp.int32)
        domains = ids[(my_half * group + inside) ^ me]

        def where_is(block):
            hit = domains == block
            return jnp.sum(jnp.where(hit, jnp.arange(1, hit.shape[1] + 1, dtype=jnp.int32), 0), 1) - 1

        other_device = me ^ group
        out_other, out_own, energy = fit_call(
            half_ints, aux_domain, aux_count, basis_domain, place, parts, coef, group_blocks, halves_packed, line, mid
        )
        shape = (group, rows, out_own.shape[2])
        got_other = lax.all_to_all(out_other.reshape(shape), GROUP, 0, 0, tiled=True)
        codes = sum_call(got_other, where_is(other_device // span), domains, positions, blocks, width)
        crossed = lax.ppermute(codes, "h", [(0, 1), (1, 0)])
        got_own = lax.all_to_all(out_own.reshape(shape), GROUP, 0, 0, tiled=True)
        sums, codes = sum_call(
            got_own, where_is(me // span), domains, positions, blocks, width, partner=crossed, energy=energy
        )
        codes = codes.reshape(blocks, rows + TAIL, span, rows).transpose(0, 2, 1, 3).reshape(devices, rows + TAIL, rows)
        arrived = lax.all_to_all(codes, AXES, 0, 0, tiled=True)
        if span == 1:
            out, total = finish_call(place, sums, arrived)
            total = total[0, 0]
        else:
            out, total = finish_plain(place, sums, arrived, span)
        return out, total / (orbitals * devices)

    return per_device


def solution(mesh):
    orb, row = mesh.devices.shape
    sizes = (2, orb // 4, 2, row // 2, 2)
    fine = Mesh(mesh.devices.reshape(sizes), AXES)
    in_specs = (P(AXES, None, None), P(AXES, None, None), P(AXES, None), P(AXES, None), P(AXES, None), P(AXES))
    return jax.shard_map(
        program(sizes), mesh=fine, in_specs=in_specs, out_specs=(P(AXES, None), P()), check_vma=False
    )
```
